32 devices in a mesh: ulysses: 8 (over z, x), blk: 4 (over y, core).
Axes of the slice: x: 2, y: 2, z: 4, core: 2. Of those that a mesh axis runs over, the one named last changes fastest.
Arguments:
- queries: bfloat16 [2048, 4096], P(('ulysses', 'blk')), may hold values from -6 to 6
- key_rows: bfloat16 [2048, 1024], P(('ulysses', 'blk')), may hold values from -6 to 6
- value_rows: bfloat16 [2048, 1024], P(('ulysses', 'blk')), may hold values from -6 to 6
Outputs:
- attended: bfloat16 [2048, 4096], P(('ulysses', 'blk'))
The draws below stay inside these ranges and needn't reach their ends.
All inputs are finite; a program needn't handle non-finite values.
Results may differ from the reference program's by a relative error of at most 0.006.
Values may be sent and summed in bfloat16 or wider, within the bound.
A program may use at most 64 MiB of HBM per device.

```python
import math
import jax
import jax.numpy as jnp
from jax import lax

Q_HEADS = 32
KV_HEADS = 8
HEAD_DIM = 128
GROUP = 4
SEQ = 2048


def draw_queries(key, part):
    raw = jax.random.normal(jax.random.fold_in(key, 1), (SEQ, Q_HEADS * HEAD_DIM), jnp.float32)
    return jnp.clip(raw, -6.0, 6.0).astype(jnp.bfloat16)


def draw_key_rows(key, part):
    raw = jax.random.normal(jax.random.fold_in(key, 3), (SEQ, KV_HEADS * HEAD_DIM), jnp.float32)
    return jnp.clip(raw, -6.0, 6.0).astype(jnp.bfloat16)


def level_of(rng, shape, cuts, smallest, high):
    def one(dim, blocks):
        steps = jax.random.uniform(jax.random.fold_in(jax.random.fold_in(rng, 6), dim), (blocks,), jnp.float32, smallest / len(cuts), high / len(cuts))
        return jnp.repeat(jnp.exp(steps), shape[dim] // blocks).reshape((-1,) + (1,) * (len(shape) - dim - 1))

    loudness = one(*cuts[0])
    for cut in cuts[1:]:
        loudness = loudness * one(*cut)
    return loudness


def centred(key, extent, scale, most, shards=(), kind=jnp.bfloat16):
    entries = jax.random.normal(key, extent, jnp.float32) * scale
    if len(shards) > 0:
        entries = level_of(key, extent, shards, -0.22, 0.18) * entries
    return jnp.clip(entries, min=-most, max=most).astype(kind)


def setup_inputs(seed: int = 0) -> dict:
    splits = jax.random.split(jax.random.key(seed), 4)
    queries = draw_queries(jax.random.fold_in(splits[3], 71), 0)
    key_rows = draw_key_rows(jax.random.fold_in(splits[3], 71), 0)
    value_rows = centred(splits[2], (SEQ, KV_HEADS * HEAD_DIM), 1.0, 6.0, ((0, 32),))
    return {"queries": queries, "key_rows": key_rows, "value_rows": value_rows}


def reference(queries, key_rows, value_rows):
    seq = queries.shape[0]
    tile_rows = min(512, seq)
    tile_count = seq // tile_rows
    scale = 1.0 / math.sqrt(HEAD_DIM)
    grouped = queries.reshape(seq, KV_HEADS, GROUP, HEAD_DIM)
    keyed = key_rows.reshape(seq, KV_HEADS, HEAD_DIM)
    valued = value_rows.reshape(seq, KV_HEADS, HEAD_DIM)
    key_where = jnp.arange(seq, dtype=jnp.int32)

    def one_tile(index):
        head = (index // tile_count).astype(jnp.int32)
        first = (index % tile_count * tile_rows).astype(jnp.int32)
        zero = jnp.zeros((), jnp.int32)
        q_part = lax.dynamic_slice(grouped, (first, head, zero, zero), (tile_rows, 1, GROUP, HEAD_DIM))[:, 0]
        k_head = lax.dynamic_slice(keyed, (zero, head, zero), (seq, 1, HEAD_DIM))[:, 0]
        v_head = lax.dynamic_slice(valued, (zero, head, zero), (seq, 1, HEAD_DIM))[:, 0]
        scores = jnp.einsum('tgd,sd->gts', q_part.astype(jnp.float32), k_head.astype(jnp.float32)) * scale
        q_where = first + jnp.arange(tile_rows, dtype=jnp.int32)
        allowed = key_where[None, :] <= q_where[:, None]
        scores = jnp.where(allowed, scores, -1e+30)
        top = lax.optimization_barrier(jnp.max(scores, axis=-1, keepdims=True))
        weights = jnp.where(allowed, jnp.exp(scores - top), 0.0)
        total = lax.optimization_barrier(jnp.sum(weights, axis=-1, keepdims=True))
        rounded = weights.astype(jnp.bfloat16)
        mixed = jnp.einsum('gts,sd->gtd', rounded.astype(jnp.float32), v_head.astype(jnp.float32)) / total
        return mixed.astype(jnp.bfloat16)
    blocks = lax.map(one_tile, jnp.arange(KV_HEADS * tile_count, dtype=jnp.int32))
    blocks = blocks.reshape(KV_HEADS, tile_count, GROUP, tile_rows, HEAD_DIM).transpose(1, 3, 0, 2, 4)
    return blocks.reshape(seq, Q_HEADS * HEAD_DIM)
```

```python
import functools
import math

import jax
import jax.numpy as jnp
from jax import lax
from jax.experimental import pallas as pl
from jax.experimental.pallas import tpu as pltpu
from jax.sharding import PartitionSpec as P

Q_HEADS = 32
KV_HEADS = 8
HEAD_DIM = 128
GROUP = Q_HEADS // KV_HEADS
MESH = pl.DeviceIdType.MESH
masked_score = -1e30


def kernel(
    ulysses, blk, q_ref, k_ref, v_ref, out_ref,
    qbuf, kbuf, vbuf, obuf, top, total, summed,
    local_sem, kv_send, kv_recv, q_send, q_recv, up_send, relay_send, up_recv, o_send, o_recv,
):
    members = KV_HEADS
    across = members // blk
    slabs = ulysses // across
    tok = q_ref.shape[0]
    rows = members * tok
    half_rows = rows // 2
    width = GROUP * HEAD_DIM
    factor = math.log2(math.e) / math.sqrt(HEAD_DIM)
    cores = 2 if blk % 2 == 0 else 1

    u = lax.axis_index("ulysses")
    b = lax.axis_index("blk")
    slab = u // across
    mx = u % across
    mine = mx * blk + b

    peers = []
    for dx in range(across):
        for dy in range(blk // cores):
            for dc in range(cores):
                px = (mx + dx) % across
                pb = (b // cores + dy) % (blk // cores) * cores + (b % cores + dc) % cores
                peers.append((px * blk + pb, (slab * across + px, pb)))
    above = (u + across, b)
    below = (u - across, b)

    barrier = pltpu.get_barrier_semaphore()
    for _, device in peers[1:]:
        pl.semaphore_signal(barrier, inc=1, device_id=device, device_id_type=MESH)

    @pl.when(slab < slabs - 1)
    def _():
        pl.semaphore_signal(barrier, inc=1, device_id=above, device_id_type=MESH)

    @pl.when(slab > 0)
    def _():
        pl.semaphore_signal(barrier, inc=1, device_id=below, device_id_type=MESH)

    neighbours = jnp.minimum(slab, 1) + jnp.minimum(slabs - 1 - slab, 1)
    pl.semaphore_wait(barrier, members - 1 + neighbours)

    def at(start, size):
        return pl.ds(pl.multiple_of(start, tok), size)

    def cols(head, size):
        return pl.ds(pl.multiple_of(head * size, size), size)

    own_rows = at(slab * rows + mine * tok, tok)
    stores = ((k_ref, kbuf), (v_ref, vbuf))

    kv_copies = []
    for i, (peer, device) in enumerate(peers):
        if i == 0:
            continue
        for which, (source, store) in enumerate(stores):
            copy = pltpu.make_async_remote_copy(
                src_ref=source.at[:, cols(peer, HEAD_DIM)],
                dst_ref=store.at[own_rows],
                send_sem=kv_send.at[i, which],
                recv_sem=kv_recv.at[mine, which],
                device_id=device,
                device_id_type=MESH,
            )
            copy.start()
            kv_copies.append(copy)
    local_copies = []
    for which, (source, store) in enumerate(stores):
        copy = pltpu.make_async_copy(
            source.at[:, cols(mine, HEAD_DIM)], store.at[own_rows], local_sem.at[which]
        )
        copy.start()
        local_copies.append(copy)
    q_copies = []
    for i, (peer, device) in enumerate(peers):
        if i == 0:
            continue
        copy = pltpu.make_async_remote_copy(
            src_ref=q_ref.at[:, cols(peer, width)],
            dst_ref=qbuf.at[at(mine * tok, tok)],
            send_sem=q_send.at[i],
            recv_sem=q_recv.at[mine],
            device_id=device,
            device_id_type=MESH,
        )
        copy.start()
        q_copies.append(copy)
    q_local = pltpu.make_async_copy(
        q_ref.at[:, cols(mine, width)], qbuf.at[at(mine * tok, tok)], local_sem.at[2]
    )
    q_local.start()

    def wait_bytes(ref, sem):
        pltpu.make_async_copy(ref, ref, sem).wait()

    def upward(i):
        peer = peers[i][0]
        where = at(slab * rows + peer * tok, tok)
        half = peer // (members // 2)
        return [
            pltpu.make_async_remote_copy(
                src_ref=store.at[where],
                dst_ref=store.at[where],
                send_sem=up_send.at[i, which],
                recv_sem=up_recv.at[slab, half, which],
                device_id=above,
                device_id_type=MESH,
            )
            for which, (_, store) in enumerate(stores)
        ]

    for i, (peer, _) in enumerate(peers):
        where = at(slab * rows + peer * tok, tok)
        for which, (_, store) in enumerate(stores):
            if i == 0:
                local_copies[which].wait()
            else:
                wait_bytes(store.at[where], kv_recv.at[peer, which])

        @pl.when(slab < slabs - 1)
        def _():
            for copy in upward(i):
                copy.start()

    def chunk_of(t):
        source = slab - 1 - t // 2
        half = (mine // (members // 2) + t % 2) % 2
        return source, half, at(source * rows + half * half_rows, half_rows)

    def relay(t):
        source, half, where = chunk_of(t)
        return [
            pltpu.make_async_remote_copy(
                src_ref=store.at[where],
                dst_ref=store.at[where],
                send_sem=relay_send.at[source, half, which],
                recv_sem=up_recv.at[source, half, which],
                device_id=above,
                device_id_type=MESH,
            )
            for which, (_, store) in enumerate(stores)
        ]

    def take(t):
        source, half, where = chunk_of(t)
        for which, (_, store) in enumerate(stores):
            wait_bytes(store.at[where], up_recv.at[source, half, which])

        @pl.when(slab < slabs - 1)
        def _():
            for copy in relay(t):
                copy.start()

    @pl.when(slab > 0)
    def _():
        take(0)
        take(1)

    q_local.wait()
    for peer, _ in peers[1:]:
        wait_bytes(qbuf.at[at(peer * tok, tok)], q_recv.at[peer])

    def block(head, q_rows, key_rows, masked, first):
        q = qbuf[q_rows, head * HEAD_DIM : (head + 1) * HEAD_DIM]
        scores = lax.dot_general(
            q, kbuf[key_rows, :], (((1,), (1,)), ((), ())), preferred_element_type=jnp.float32
        ) * factor
        if masked:
            down = lax.broadcasted_iota(jnp.int32, scores.shape, 0)
            right = lax.broadcasted_iota(jnp.int32, scores.shape, 1)
            scores = jnp.where(right <= down, scores, masked_score)
        peak = jnp.max(scores, axis=1, keepdims=True)
        size = scores.shape[0]
        if first:
            new_top = jnp.broadcast_to(peak, (size, HEAD_DIM))
        else:
            old_top = top[head, q_rows]
            new_top = jnp.maximum(old_top, peak)
        repeats = scores.shape[1] // HEAD_DIM
        weights = jnp.exp2(scores - jnp.concatenate([new_top] * repeats, axis=1))
        if masked:
            weights = jnp.where(right <= down, weights, 0.0)
        part = weights[:, :HEAD_DIM]
        for r in range(1, repeats):
            part = part + weights[:, r * HEAD_DIM : (r + 1) * HEAD_DIM]
        mixed = jnp.dot(
            weights.astype(jnp.bfloat16), vbuf[key_rows, :], preferred_element_type=jnp.float32
        )
        if first:
            total[head, q_rows] = part
            summed[head, q_rows] = mixed
        else:
            shrink = jnp.exp2(old_top - new_top)
            total[head, q_rows] = total[head, q_rows] * shrink + part
            summed[head, q_rows] = summed[head, q_rows] * shrink + mixed
        top[head, q_rows] = new_top

    low, high = pl.ds(0, half_rows), pl.ds(half_rows, half_rows)
    own_low = at(slab * rows, half_rows)
    own_high = at(slab * rows + half_rows, half_rows)
    for head in range(GROUP):
        block(head, low, own_low, True, True)
        block(head, high, own_low, False, True)
        block(head, high, own_high, True, False)

    def visit(t, carry):
        @pl.when(t >= 2)
        def _():
            take(t)

        where = chunk_of(t)[2]
        for head in range(GROUP):
            for q_rows in (low, high):
                block(head, q_rows, where, False, False)
        return carry

    lax.fori_loop(0, 2 * slab, visit, 0)

    def finish(peer):
        where = at(peer * tok, tok)
        for head in range(GROUP):
            sums = jnp.sum(total[head, where], axis=1, keepdims=True)
            obuf[where, head * HEAD_DIM : (head + 1) * HEAD_DIM] = (
                summed[head, where] / sums
            ).astype(jnp.bfloat16)

    o_copies = []
    for i in reversed(range(1, members)):
        peer, device = peers[i]
        finish(peer)
        copy = pltpu.make_async_remote_copy(
            src_ref=obuf.at[at(peer * tok, tok)],
            dst_ref=out_ref.at[:, cols(mine, width)],
            send_sem=o_send.at[i],
            recv_sem=o_recv.at[mine],
            device_id=device,
            device_id_type=MESH,
        )
        copy.start()
        o_copies.append(copy)
    finish(mine)
    o_local = pltpu.make_async_copy(
        obuf.at[at(mine * tok, tok)], out_ref.at[:, cols(mine, width)], local_sem.at[3]
    )
    o_local.start()

    for copy in kv_copies + q_copies:
        copy.wait_send()

    @pl.when(slab < slabs - 1)
    def _():
        for i in range(members):
            for copy in upward(i):
                copy.wait_send()

        def sent(t, carry):
            for copy in relay(t):
                copy.wait_send()
            return carry

        lax.fori_loop(0, 2 * slab, sent, 0)

    for copy in o_copies:
        copy.wait_send()
    o_local.wait()
    for peer, _ in peers[1:]:
        wait_bytes(out_ref.at[:, cols(peer, width)], o_recv.at[peer])


def solution(mesh):
    ulysses, blk = mesh.shape["ulysses"], mesh.shape["blk"]
    members = KV_HEADS
    assert members % blk == 0 and ulysses % (members // blk) == 0
    slabs = ulysses // (members // blk)

    def per_device(queries, key_rows, value_rows):
        tok = queries.shape[0]
        rows = members * tok
        seq = slabs * rows
        dma = pltpu.SemaphoreType.DMA
        return pl.pallas_call(
            functools.partial(kernel, ulysses, blk),
            out_shape=jax.ShapeDtypeStruct(queries.shape, queries.dtype),
            in_specs=[pl.BlockSpec(memory_space=pltpu.VMEM)] * 3,
            out_specs=pl.BlockSpec(memory_space=pltpu.VMEM),
            scratch_shapes=[
                pltpu.VMEM((rows, GROUP * HEAD_DIM), jnp.bfloat16),
                pltpu.VMEM((seq, HEAD_DIM), jnp.bfloat16),
                pltpu.VMEM((seq, HEAD_DIM), jnp.bfloat16),
                pltpu.VMEM((rows, GROUP * HEAD_DIM), jnp.bfloat16),
                pltpu.VMEM((GROUP, rows, HEAD_DIM), jnp.float32),
                pltpu.VMEM((GROUP, rows, HEAD_DIM), jnp.float32),
                pltpu.VMEM((GROUP, rows, HEAD_DIM), jnp.float32),
                dma((4,)),
                dma((members, 2)),
                dma((members, 2)),
                dma((members,)),
                dma((members,)),
                dma((members, 2)),
                dma((slabs, 2, 2)),
                dma((slabs, 2, 2)),
                dma((members,)),
                dma((members,)),
            ],
            compiler_params=pltpu.CompilerParams(collective_id=0, has_side_effects=True),
        )(queries, key_rows, value_rows)

    spec = P(("ulysses", "blk"), None)
    return jax.shard_map(
        per_device, mesh=mesh, in_specs=(spec, spec, spec), out_specs=spec, check_vma=False
    )
```

```python
import functools
import math

import jax
import jax.numpy as jnp
from jax import lax
from jax.experimental import pallas as pl
from jax.experimental.pallas import tpu as pltpu
from jax.sharding import PartitionSpec as P

Q_HEADS = 32
KV_HEADS = 8
HEAD_DIM = 128
GROUP = Q_HEADS // KV_HEADS
MESH = pl.DeviceIdType.MESH
masked_score = -1e30


def kernel(
    ulysses, blk, q_hbm, k_hbm, v_hbm, out_ref,
    q_ref, k_ref, v_ref,
    qbuf, kbuf, vbuf, obuf, top, total, summed,
    local_sem, kv_send, kv_recv, q_send, q_recv, up_send, relay_send, up_recv, o_send, o_recv, go_sem,
):
    members = KV_HEADS
    across = members // blk
    slabs = ulysses // across
    tok = q_ref.shape[0]
    loads = [
        pltpu.make_async_copy(source, store, local_sem.at[4 + i])
        for i, (source, store) in enumerate(((k_hbm, k_ref), (v_hbm, v_ref), (q_hbm, q_ref)))
    ]
    for load in loads:
        load.start()
    rows = members * tok
    half_rows = rows // 2
    width = GROUP * HEAD_DIM
    factor = math.log2(math.e) / math.sqrt(HEAD_DIM)
    cores = 2 if blk % 2 == 0 else 1

    u = lax.axis_index("ulysses")
    b = lax.axis_index("blk")
    slab = u // across
    mx = u % across
    mine = mx * blk + b

    peers = []
    for dx in range(across):
        for dy in range(blk // cores):
            for dc in range(cores):
                core = (b % cores + dc) % cores if dx == dy == 0 else dc
                px = (mx + dx) % across
                pb = (b // cores + dy) % (blk // cores) * cores + core
                peers.append((px * blk + pb, (slab * across + px, pb)))
    lead = b % cores == 0
    partner = peers[cores - 1][1]
    turns = list(range(1, cores)) + [i for c in range(cores) for i in range(cores + c, members, cores)]
    above = (u + across, b)
    below = (u - across, b)

    barrier = pltpu.get_barrier_semaphore()
    for _, device in peers[1:]:
        pl.semaphore_signal(barrier, inc=1, device_id=device, device_id_type=MESH)

    @pl.when(slab < slabs - 1)
    def _():
        pl.semaphore_signal(barrier, inc=1, device_id=above, device_id_type=MESH)

    @pl.when(slab > 0)
    def _():
        pl.semaphore_signal(barrier, inc=1, device_id=below, device_id_type=MESH)

    neighbours = jnp.minimum(slab, 1) + jnp.minimum(slabs - 1 - slab, 1)
    pl.semaphore_wait(barrier, members - 1 + neighbours)

    def at(start, size):
        return pl.ds(pl.multiple_of(start, tok), size)

    def cols(head, size):
        return pl.ds(pl.multiple_of(head * size, size), size)

    own_rows = at(slab * rows + mine * tok, tok)
    stores = ((k_ref, kbuf), (v_ref, vbuf))

    kv_copies = []
    for load in loads[:2]:
        load.wait()
    for i in turns:
        peer, device = peers[i]
        for which, (source, store) in enumerate(stores):
            copy = pltpu.make_async_remote_copy(
                src_ref=source.at[:, cols(peer, HEAD_DIM)],
                dst_ref=store.at[own_rows],
                send_sem=kv_send.at[i, which],
                recv_sem=kv_recv.at[mine, which],
                device_id=device,
                device_id_type=MESH,
            )
            copy.start()
            kv_copies.append(copy)
    local_copies = []
    for which, (source, store) in enumerate(stores):
        copy = pltpu.make_async_copy(
            source.at[:, cols(mine, HEAD_DIM)], store.at[own_rows], local_sem.at[which]
        )
        copy.start()
        local_copies.append(copy)
    q_copies = []
    loads[2].wait()
    for i in turns:
        peer, device = peers[i]
        copy = pltpu.make_async_remote_copy(
            src_ref=q_ref.at[:, cols(peer, width)],
            dst_ref=qbuf.at[at(mine * tok, tok)],
            send_sem=q_send.at[i],
            recv_sem=q_recv.at[mine],
            device_id=device,
            device_id_type=MESH,
        )
        copy.start()
        q_copies.append(copy)
    q_local = pltpu.make_async_copy(
        q_ref.at[:, cols(mine, width)], qbuf.at[at(mine * tok, tok)], local_sem.at[2]
    )
    q_local.start()

    def wait_bytes(ref, sem):
        pltpu.make_async_copy(ref, ref, sem).wait()

    def upward(i):
        peer = peers[i][0]
        where = at(slab * rows + peer * tok, tok)
        half = peer // (members // 2)
        return [
            pltpu.make_async_remote_copy(
                src_ref=store.at[where],
                dst_ref=store.at[where],
                send_sem=up_send.at[i, which],
                recv_sem=up_recv.at[slab, half, which],
                device_id=above,
                device_id_type=MESH,
            )
            for which, (_, store) in enumerate(stores)
        ]

    for i, (peer, _) in enumerate(peers):
        where = at(slab * rows + peer * tok, tok)
        for which, (_, store) in enumerate(stores):
            if i == 0:
                local_copies[which].wait()
            else:
                wait_bytes(store.at[where], kv_recv.at[peer, which])

        @pl.when((slab < slabs - 1) & lead)
        def _():
            for copy in upward(i):
                copy.start()

    def chunk_of(t):
        source = slab - 1 - t // 2
        half = (mine // (members // 2) + t % 2) % 2
        return source, half, at(source * rows + half * half_rows, half_rows)

    def relay(t):
        source, half, where = chunk_of(t)
        return [
            pltpu.make_async_remote_copy(
                src_ref=store.at[where],
                dst_ref=store.at[where],
                send_sem=relay_send.at[source, half, which],
                recv_sem=up_recv.at[source, half, which],
                device_id=above,
                device_id_type=MESH,
            )
            for which, (_, store) in enumerate(stores)
        ]

    def take(t):
        source, half, where = chunk_of(t)
        for which, (_, store) in enumerate(stores):
            wait_bytes(store.at[where], up_recv.at[source, half, which])

        @pl.when(slab < slabs - 1)
        def _():
            for copy in relay(t):
                copy.start()

    ahead = 4

    def pass_on():
        if cores > 1:
            @pl.when(slab < slabs - 1)
            def _():
                pl.semaphore_signal(go_sem, inc=1, device_id=partner, device_id_type=MESH)

    def take_one(t, carry):
        take(t)
        return carry

    @pl.when(lead)
    def _():
        lax.fori_loop(0, jnp.minimum(ahead, 2 * slab), take_one, 0)

        @pl.when(2 * slab <= ahead)
        def _():
            pass_on()

    if cores > 1:
        @pl.when((slab < slabs - 1) & (b % cores != 0))
        def _():
            pl.semaphore_wait(go_sem, 1)
            for i in range(members):
                for copy in upward(i):
                    copy.start()

    q_local.wait()
    for peer, _ in peers[1:]:
        wait_bytes(qbuf.at[at(peer * tok, tok)], q_recv.at[peer])

    def block(head, q_rows, key_rows, masked, first):
        q = qbuf[q_rows, head * HEAD_DIM : (head + 1) * HEAD_DIM]
        scores = lax.dot_general(
            q, kbuf[key_rows, :], (((1,), (1,)), ((), ())), preferred_element_type=jnp.float32
        ) * factor
        if masked:
            down = lax.broadcasted_iota(jnp.int32, scores.shape, 0)
            right = lax.broadcasted_iota(jnp.int32, scores.shape, 1)
            scores = jnp.where(right <= down, scores, masked_score)
        peak = jnp.max(scores, axis=1, keepdims=True)
        size = scores.shape[0]
        if first:
            new_top = jnp.broadcast_to(peak, (size, HEAD_DIM))
        else:
            old_top = top[head, q_rows]
            new_top = jnp.maximum(old_top, peak)
        repeats = scores.shape[1] // HEAD_DIM
        weights = jnp.exp2(scores - jnp.concatenate([new_top] * repeats, axis=1))
        if masked:
            weights = jnp.where(right <= down, weights, 0.0)
        part = weights[:, :HEAD_DIM]
        for r in range(1, repeats):
            part = part + weights[:, r * HEAD_DIM : (r + 1) * HEAD_DIM]
        mixed = jnp.dot(
            weights.astype(jnp.bfloat16), vbuf[key_rows, :], preferred_element_type=jnp.float32
        )
        if first:
            total[head, q_rows] = part
            summed[head, q_rows] = mixed
        else:
            shrink = jnp.exp2(old_top - new_top)
            total[head, q_rows] = total[head, q_rows] * shrink + part
            summed[head, q_rows] = summed[head, q_rows] * shrink + mixed
        top[head, q_rows] = new_top

    low, high = pl.ds(0, half_rows), pl.ds(half_rows, half_rows)
    own_low = at(slab * rows, half_rows)
    own_high = at(slab * rows + half_rows, half_rows)
    for head in range(GROUP):
        block(head, low, own_low, True, True)
        block(head, high, own_low, False, True)
        block(head, high, own_high, True, False)

    def visit(t, carry):
        @pl.when((t >= ahead) | (b % cores != 0))
        def _():
            take(t)

        @pl.when((t >= ahead) & (t == 2 * slab - 1) & lead)
        def _():
            pass_on()

        where = chunk_of(t)[2]
        for head in range(GROUP):
            for q_rows in (low, high):
                block(head, q_rows, where, False, False)
        return carry

    lax.fori_loop(0, 2 * slab, visit, 0)

    def finish(peer):
        where = at(peer * tok, tok)
        for head in range(GROUP):
            sums = jnp.sum(total[head, where], axis=1, keepdims=True)
            obuf[where, head * HEAD_DIM : (head + 1) * HEAD_DIM] = (
                summed[head, where] / sums
            ).astype(jnp.bfloat16)

    o_copies = []
    for i in reversed(range(1, members)):
        peer, device = peers[i]
        finish(peer)
        copy = pltpu.make_async_remote_copy(
            src_ref=obuf.at[at(peer * tok, tok)],
            dst_ref=out_ref.at[:, cols(mine, width)],
            send_sem=o_send.at[i],
            recv_sem=o_recv.at[mine],
            device_id=device,
            device_id_type=MESH,
        )
        copy.start()
        o_copies.append(copy)
    finish(mine)
    o_local = pltpu.make_async_copy(
        obuf.at[at(mine * tok, tok)], out_ref.at[:, cols(mine, width)], local_sem.at[3]
    )
    o_local.start()

    for copy in kv_copies + q_copies:
        copy.wait_send()

    @pl.when(slab < slabs - 1)
    def _():
        for i in range(members):
            for copy in upward(i):
                copy.wait_send()

        def sent(t, carry):
            for copy in relay(t):
                copy.wait_send()
            return carry

        lax.fori_loop(0, 2 * slab, sent, 0)

    for copy in o_copies:
        copy.wait_send()
    o_local.wait()
    for peer, _ in peers[1:]:
        wait_bytes(out_ref.at[:, cols(peer, width)], o_recv.at[peer])


def solution(mesh):
    ulysses, blk = mesh.shape["ulysses"], mesh.shape["blk"]
    members = KV_HEADS
    assert members % blk == 0 and ulysses % (members // blk) == 0
    slabs = ulysses // (members // blk)

    def per_device(queries, key_rows, value_rows):
        tok = queries.shape[0]
        rows = members * tok
        seq = slabs * rows
        dma = pltpu.SemaphoreType.DMA
        return pl.pallas_call(
            functools.partial(kernel, ulysses, blk),
            out_shape=jax.ShapeDtypeStruct(queries.shape, queries.dtype),
            in_specs=[pl.BlockSpec(memory_space=pl.ANY)] * 3,
            out_specs=pl.BlockSpec(memory_space=pl.ANY),
            scratch_shapes=[
                pltpu.VMEM(queries.shape, queries.dtype),
                pltpu.VMEM(key_rows.shape, key_rows.dtype),
                pltpu.VMEM(value_rows.shape, value_rows.dtype),
                pltpu.VMEM((rows, GROUP * HEAD_DIM), jnp.bfloat16),
                pltpu.VMEM((seq, HEAD_DIM), jnp.bfloat16),
                pltpu.VMEM((seq, HEAD_DIM), jnp.bfloat16),
                pltpu.VMEM((rows, GROUP * HEAD_DIM), jnp.bfloat16),
                pltpu.VMEM((GROUP, rows, HEAD_DIM), jnp.float32),
                pltpu.VMEM((GROUP, rows, HEAD_DIM), jnp.float32),
                pltpu.VMEM((GROUP, rows, HEAD_DIM), jnp.float32),
                dma((7,)),
                dma((members, 2)),
                dma((members, 2)),
                dma((members,)),
                dma((members,)),
                dma((members, 2)),
                dma((slabs, 2, 2)),
                dma((slabs, 2, 2)),
                dma((members,)),
                dma((members,)),
                pltpu.SemaphoreType.REGULAR,
            ],
            compiler_params=pltpu.CompilerParams(collective_id=0, has_side_effects=True),
        )(queries, key_rows, value_rows)

    spec = P(("ulysses", "blk"), None)
    return jax.shard_map(
        per_device, mesh=mesh, in_specs=(spec, spec, spec), out_specs=spec, check_vma=False
    )
```

```python
import functools
import math

import jax
import jax.numpy as jnp
from jax import lax
from jax.experimental import pallas as pl
from jax.experimental.pallas import tpu as pltpu
from jax.sharding import PartitionSpec as P

Q_HEADS = 32
KV_HEADS = 8
HEAD_DIM = 128
GROUP = Q_HEADS // KV_HEADS
MESH = pl.DeviceIdType.MESH
masked_score = -1e30


def kernel(
    ulysses, blk, q_hbm, k_hbm, v_hbm, out_ref,
    q_ref, k_ref, v_ref,
    qbuf, kbuf, vbuf, obuf, top, total, summed,
    local_sem, kv_send, kv_recv, q_send, q_recv, up_send, relay_send, up_recv, o_send, o_recv, go_sem,
):
    members = KV_HEADS
    across = members // blk
    slabs = ulysses // across
    tok = q_ref.shape[0]
    loads = [
        pltpu.make_async_copy(source, store, local_sem.at[4 + i])
        for i, (source, store) in enumerate(((k_hbm, k_ref), (v_hbm, v_ref), (q_hbm, q_ref)))
    ]
    for load in loads:
        load.start()
    rows = members * tok
    half_rows = rows // 2
    width = GROUP * HEAD_DIM
    factor = math.log2(math.e) / math.sqrt(HEAD_DIM)
    cores = 2 if blk % 2 == 0 else 1

    u = lax.axis_index("ulysses")
    b = lax.axis_index("blk")
    slab = u // across
    mx = u % across
    mine = mx * blk + b

    peers = []
    for dx in range(across):
        for dy in range(blk // cores):
            for dc in range(cores):
                core = (b % cores + dc) % cores if dx == dy == 0 else dc
                px = (mx + dx) % across
                pb = (b // cores + dy) % (blk // cores) * cores + core
                peers.append((px * blk + pb, (slab * across + px, pb)))
    lead = b % cores == 0
    partner = peers[cores - 1][1]
    turns = list(range(1, cores)) + [i for c in range(cores) for i in range(cores + c, members, cores)]
    above = (u + across, b)
    below = (u - across, b)

    barrier = pltpu.get_barrier_semaphore()
    for _, device in peers[1:]:
        pl.semaphore_signal(barrier, inc=1, device_id=device, device_id_type=MESH)

    @pl.when(slab < slabs - 1)
    def _():
        pl.semaphore_signal(barrier, inc=1, device_id=above, device_id_type=MESH)

    @pl.when(slab > 0)
    def _():
        pl.semaphore_signal(barrier, inc=1, device_id=below, device_id_type=MESH)

    neighbours = jnp.minimum(slab, 1) + jnp.minimum(slabs - 1 - slab, 1)
    pl.semaphore_wait(barrier, members - 1 + neighbours)

    def at(start, size):
        return pl.ds(pl.multiple_of(start, tok), size)

    def cols(head, size):
        return pl.ds(pl.multiple_of(head * size, size), size)

    own_rows = at(slab * rows + mine * tok, tok)
    stores = ((k_ref, kbuf), (v_ref, vbuf))

    kv_copies = []
    for load in loads[:2]:
        load.wait()
    for i in turns:
        peer, device = peers[i]
        for which, (source, store) in enumerate(stores):
            copy = pltpu.make_async_remote_copy(
                src_ref=source.at[:, cols(peer, HEAD_DIM)],
                dst_ref=store.at[own_rows],
                send_sem=kv_send.at[i, which],
                recv_sem=kv_recv.at[mine, which],
                device_id=device,
                device_id_type=MESH,
            )
            copy.start()
            kv_copies.append(copy)
    local_copies = []
    for which, (source, store) in enumerate(stores):
        copy = pltpu.make_async_copy(
            source.at[:, cols(mine, HEAD_DIM)], store.at[own_rows], local_sem.at[which]
        )
        copy.start()
        local_copies.append(copy)
    q_copies = []
    loads[2].wait()
    for i in turns:
        peer, device = peers[i]
        copy = pltpu.make_async_remote_copy(
            src_ref=q_ref.at[:, cols(peer, width)],
            dst_ref=qbuf.at[at(mine * tok, tok)],
            send_sem=q_send.at[i],
            recv_sem=q_recv.at[mine],
            device_id=device,
            device_id_type=MESH,
        )
        copy.start()
        q_copies.append(copy)
    q_local = pltpu.make_async_copy(
        q_ref.at[:, cols(mine, width)], qbuf.at[at(mine * tok, tok)], local_sem.at[2]
    )
    q_local.start()

    def wait_bytes(ref, sem):
        pltpu.make_async_copy(ref, ref, sem).wait()

    def upward(i):
        peer = peers[i][0]
        where = at(slab * rows + peer * tok, tok)
        half = peer // (members // 2)
        return [
            pltpu.make_async_remote_copy(
                src_ref=store.at[where],
                dst_ref=store.at[where],
                send_sem=up_send.at[i, which],
                recv_sem=up_recv.at[slab, half, which],
                device_id=above,
                device_id_type=MESH,
            )
            for which, (_, store) in enumerate(stores)
        ]

    for i, (peer, _) in enumerate(peers):
        where = at(slab * rows + peer * tok, tok)
        for which, (_, store) in enumerate(stores):
            if i == 0:
                local_copies[which].wait()
            else:
                wait_bytes(store.at[where], kv_recv.at[peer, which])

        @pl.when(slab < slabs - 1)
        def _():
            for copy in upward(i):
                copy.start()

    def chunk_of(t):
        source = slab - 1 - t // 2
        half = (mine // (members // 2) + t % 2) % 2
        return source, half, at(source * rows + half * half_rows, half_rows)

    def relay(t):
        source, half, where = chunk_of(t)
        return [
            pltpu.make_async_remote_copy(
                src_ref=store.at[where],
                dst_ref=store.at[where],
                send_sem=relay_send.at[source, half, which],
                recv_sem=up_recv.at[source, half, which],
                device_id=above,
                device_id_type=MESH,
            )
            for which, (_, store) in enumerate(stores)
        ]

    def take(t):
        source, half, where = chunk_of(t)
        for which, (_, store) in enumerate(stores):
            wait_bytes(store.at[where], up_recv.at[source, half, which])

        @pl.when(slab < slabs - 1)
        def _():
            for copy in relay(t):
                copy.start()

    relaying = (slab > 0) & (slab < slabs - 1)
    if cores > 1:
        @pl.when(relaying & (b % cores != 0))
        def _():
            pl.semaphore_wait(go_sem, 1)

    @pl.when(slab > 0)
    def _():
        take(0)
        take(1)

    if cores > 1:
        @pl.when(relaying & lead)
        def _():
            pl.semaphore_signal(go_sem, inc=1, device_id=partner, device_id_type=MESH)

    q_local.wait()
    for peer, _ in peers[1:]:
        wait_bytes(qbuf.at[at(peer * tok, tok)], q_recv.at[peer])

    def block(head, q_rows, key_rows, masked, first):
        q = qbuf[q_rows, head * HEAD_DIM : (head + 1) * HEAD_DIM]
        scores = lax.dot_general(
            q, kbuf[key_rows, :], (((1,), (1,)), ((), ())), preferred_element_type=jnp.float32
        ) * factor
        if masked:
            down = lax.broadcasted_iota(jnp.int32, scores.shape, 0)
            right = lax.broadcasted_iota(jnp.int32, scores.shape, 1)
            scores = jnp.where(right <= down, scores, masked_score)
        peak = jnp.max(scores, axis=1, keepdims=True)
        size = scores.shape[0]
        if first:
            new_top = jnp.broadcast_to(peak, (size, HEAD_DIM))
        else:
            old_top = top[head, q_rows]
            new_top = jnp.maximum(old_top, peak)
        repeats = scores.shape[1] // HEAD_DIM
        weights = jnp.exp2(scores - jnp.concatenate([new_top] * repeats, axis=1))
        if masked:
            weights = jnp.where(right <= down, weights, 0.0)
        part = weights[:, :HEAD_DIM]
        for r in range(1, repeats):
            part = part + weights[:, r * HEAD_DIM : (r + 1) * HEAD_DIM]
        mixed = jnp.dot(
            weights.astype(jnp.bfloat16), vbuf[key_rows, :], preferred_element_type=jnp.float32
        )
        if first:
            total[head, q_rows] = part
            summed[head, q_rows] = mixed
        else:
            shrink = jnp.exp2(old_top - new_top)
            total[head, q_rows] = total[head, q_rows] * shrink + part
            summed[head, q_rows] = summed[head, q_rows] * shrink + mixed
        top[head, q_rows] = new_top

    low, high = pl.ds(0, half_rows), pl.ds(half_rows, half_rows)
    own_low = at(slab * rows, half_rows)
    own_high = at(slab * rows + half_rows, half_rows)
    for head in range(GROUP):
        block(head, low, own_low, True, True)
        block(head, high, own_low, False, True)
        block(head, high, own_high, True, False)

    def visit(t, carry):
        @pl.when(t >= 2)
        def _():
            take(t)

        where = chunk_of(t)[2]
        for head in range(GROUP):
            for q_rows in (low, high):
                block(head, q_rows, where, False, False)
        return carry

    lax.fori_loop(0, 2 * slab, visit, 0)

    def finish(peer):
        where = at(peer * tok, tok)
        for head in range(GROUP):
            sums = jnp.sum(total[head, where], axis=1, keepdims=True)
            obuf[where, head * HEAD_DIM : (head + 1) * HEAD_DIM] = (
                summed[head, where] / sums
            ).astype(jnp.bfloat16)

    o_copies = []
    for i in reversed(range(1, members)):
        peer, device = peers[i]
        finish(peer)
        copy = pltpu.make_async_remote_copy(
            src_ref=obuf.at[at(peer * tok, tok)],
            dst_ref=out_ref.at[:, cols(mine, width)],
            send_sem=o_send.at[i],
            recv_sem=o_recv.at[mine],
            device_id=device,
            device_id_type=MESH,
        )
        copy.start()
        o_copies.append(copy)
    finish(mine)
    o_local = pltpu.make_async_copy(
        obuf.at[at(mine * tok, tok)], out_ref.at[:, cols(mine, width)], local_sem.at[3]
    )
    o_local.start()

    for copy in kv_copies + q_copies:
        copy.wait_send()

    @pl.when(slab < slabs - 1)
    def _():
        for i in range(members):
            for copy in upward(i):
                copy.wait_send()

        def sent(t, carry):
            for copy in relay(t):
                copy.wait_send()
            return carry

        lax.fori_loop(0, 2 * slab, sent, 0)

    for copy in o_copies:
        copy.wait_send()
    o_local.wait()
    for peer, _ in peers[1:]:
        wait_bytes(out_ref.at[:, cols(peer, width)], o_recv.at[peer])


def solution(mesh):
    ulysses, blk = mesh.shape["ulysses"], mesh.shape["blk"]
    members = KV_HEADS
    assert members % blk == 0 and ulysses % (members // blk) == 0
    slabs = ulysses // (members // blk)

    def per_device(queries, key_rows, value_rows):
        tok = queries.shape[0]
        rows = members * tok
        seq = slabs * rows
        dma = pltpu.SemaphoreType.DMA
        return pl.pallas_call(
            functools.partial(kernel, ulysses, blk),
            out_shape=jax.ShapeDtypeStruct(queries.shape, queries.dtype),
            in_specs=[pl.BlockSpec(memory_space=pl.ANY)] * 3,
            out_specs=pl.BlockSpec(memory_space=pl.ANY),
            scratch_shapes=[
                pltpu.VMEM(queries.shape, queries.dtype),
                pltpu.VMEM(key_rows.shape, key_rows.dtype),
                pltpu.VMEM(value_rows.shape, value_rows.dtype),
                pltpu.VMEM((rows, GROUP * HEAD_DIM), jnp.bfloat16),
                pltpu.VMEM((seq, HEAD_DIM), jnp.bfloat16),
                pltpu.VMEM((seq, HEAD_DIM), jnp.bfloat16),
                pltpu.VMEM((rows, GROUP * HEAD_DIM), jnp.bfloat16),
                pltpu.VMEM((GROUP, rows, HEAD_DIM), jnp.float32),
                pltpu.VMEM((GROUP, rows, HEAD_DIM), jnp.float32),
                pltpu.VMEM((GROUP, rows, HEAD_DIM), jnp.float32),
                dma((7,)),
                dma((members, 2)),
                dma((members, 2)),
                dma((members,)),
                dma((members,)),
                dma((members, 2)),
                dma((slabs, 2, 2)),
                dma((slabs, 2, 2)),
                dma((members,)),
                dma((members,)),
                pltpu.SemaphoreType.REGULAR,
            ],
            compiler_params=pltpu.CompilerParams(collective_id=0, has_side_effects=True),
        )(queries, key_rows, value_rows)

    spec = P(("ulysses", "blk"), None)
    return jax.shard_map(
        per_device, mesh=mesh, in_specs=(spec, spec, spec), out_specs=spec, check_vma=False
    )
```

```python
import functools
import math

import jax
import jax.numpy as jnp
from jax import lax
from jax.experimental import pallas as pl
from jax.experimental.pallas import tpu as pltpu
from jax.sharding import PartitionSpec as P

Q_HEADS = 32
KV_HEADS = 8
HEAD_DIM = 128
GROUP = Q_HEADS // KV_HEADS
MESH = pl.DeviceIdType.MESH
masked_score = -1e30


def kernel(
    ulysses, blk, q_hbm, k_hbm, v_hbm, out_ref,
    q_ref, k_ref, v_ref,
    qbuf, kbuf, vbuf, obuf, top, total, summed,
    local_sem, kv_send, kv_recv, q_send, q_recv, up_send, relay_send, up_recv, o_send, o_recv, go_sem,
):
    members = KV_HEADS
    across = members // blk
    slabs = ulysses // across
    tok = q_ref.shape[0]
    loads = [
        pltpu.make_async_copy(source, store, local_sem.at[4 + i])
        for i, (source, store) in enumerate(((k_hbm, k_ref), (v_hbm, v_ref), (q_hbm, q_ref)))
    ]
    for load in loads:
        load.start()
    rows = members * tok
    half_rows = rows // 2
    width = GROUP * HEAD_DIM
    factor = math.log2(math.e) / math.sqrt(HEAD_DIM)
    cores = 2 if blk % 2 == 0 else 1

    u = lax.axis_index("ulysses")
    b = lax.axis_index("blk")
    slab = u // across
    mx = u % across
    mine = mx * blk + b

    peers = []
    for dx in range(across):
        for dy in range(blk // cores):
            for dc in range(cores):
                core = (b % cores + dc) % cores if dx == dy == 0 else dc
                px = (mx + dx) % across
                pb = (b // cores + dy) % (blk // cores) * cores + core
                peers.append((px * blk + pb, (slab * across + px, pb)))
    lead = b % cores == 0
    partner = peers[cores - 1][1]
    turns = list(range(1, cores)) + [i for c in range(cores) for i in range(cores + c, members, cores)]
    above = (u + across, b)
    below = (u - across, b)

    barrier = pltpu.get_barrier_semaphore()
    for _, device in peers[1:]:
        pl.semaphore_signal(barrier, inc=1, device_id=device, device_id_type=MESH)

    @pl.when(slab < slabs - 1)
    def _():
        pl.semaphore_signal(barrier, inc=1, device_id=above, device_id_type=MESH)

    @pl.when(slab > 0)
    def _():
        pl.semaphore_signal(barrier, inc=1, device_id=below, device_id_type=MESH)

    neighbours = jnp.minimum(slab, 1) + jnp.minimum(slabs - 1 - slab, 1)
    pl.semaphore_wait(barrier, members - 1 + neighbours)

    def at(start, size):
        return pl.ds(pl.multiple_of(start, tok), size)

    def cols(head, size):
        return pl.ds(pl.multiple_of(head * size, size), size)

    own_rows = at(slab * rows + mine * tok, tok)
    stores = ((k_ref, kbuf), (v_ref, vbuf))

    kv_copies = []
    for load in loads[:2]:
        load.wait()
    for i in turns:
        peer, device = peers[i]
        for which, (source, store) in enumerate(stores):
            copy = pltpu.make_async_remote_copy(
                src_ref=source.at[:, cols(peer, HEAD_DIM)],
                dst_ref=store.at[own_rows],
                send_sem=kv_send.at[i, which],
                recv_sem=kv_recv.at[mine, which],
                device_id=device,
                device_id_type=MESH,
            )
            copy.start()
            kv_copies.append(copy)
    local_copies = []
    for which, (source, store) in enumerate(stores):
        copy = pltpu.make_async_copy(
            source.at[:, cols(mine, HEAD_DIM)], store.at[own_rows], local_sem.at[which]
        )
        copy.start()
        local_copies.append(copy)
    q_copies = []
    loads[2].wait()
    for i in turns:
        peer, device = peers[i]
        copy = pltpu.make_async_remote_copy(
            src_ref=q_ref.at[:, cols(peer, width)],
            dst_ref=qbuf.at[at(mine * tok, tok)],
            send_sem=q_send.at[i],
            recv_sem=q_recv.at[mine],
            device_id=device,
            device_id_type=MESH,
        )
        copy.start()
        q_copies.append(copy)
    q_local = pltpu.make_async_copy(
        q_ref.at[:, cols(mine, width)], qbuf.at[at(mine * tok, tok)], local_sem.at[2]
    )
    q_local.start()

    def wait_bytes(ref, sem):
        pltpu.make_async_copy(ref, ref, sem).wait()

    def upward(i):
        peer = peers[i][0]
        where = at(slab * rows + peer * tok, tok)
        half = peer // (members // 2)
        return [
            pltpu.make_async_remote_copy(
                src_ref=store.at[where],
                dst_ref=store.at[where],
                send_sem=up_send.at[i, which],
                recv_sem=up_recv.at[slab, half, which],
                device_id=above,
                device_id_type=MESH,
            )
            for which, (_, store) in enumerate(stores)
        ]

    for i, (peer, _) in enumerate(peers):
        where = at(slab * rows + peer * tok, tok)
        for which, (_, store) in enumerate(stores):
            if i == 0:
                local_copies[which].wait()
            else:
                wait_bytes(store.at[where], kv_recv.at[peer, which])

        @pl.when(slab < slabs - 1)
        def _():
            for copy in upward(i):
                copy.start()

    def chunk_of(t):
        source = slab - 1 - t // 2
        half = (mine // (members // 2) + t % 2) % 2
        return source, half, at(source * rows + half * half_rows, half_rows)

    def relay(t):
        source, half, where = chunk_of(t)
        return [
            pltpu.make_async_remote_copy(
                src_ref=store.at[where],
                dst_ref=store.at[where],
                send_sem=relay_send.at[source, half, which],
                recv_sem=up_recv.at[source, half, which],
                device_id=above,
                device_id_type=MESH,
            )
            for which, (_, store) in enumerate(stores)
        ]

    def take(t):
        source, half, where = chunk_of(t)
        for which, (_, store) in enumerate(stores):
            wait_bytes(store.at[where], up_recv.at[source, half, which])

        @pl.when(slab < slabs - 1)
        def _():
            for copy in relay(t):
                copy.start()

    relaying = (slab > 0) & (slab < slabs - 1)
    if cores > 1:
        @pl.when(relaying & (b % cores != 0))
        def _():
            pl.semaphore_wait(go_sem, 1)

    @pl.when(slab > 0)
    def _():
        take(0)
        take(1)

    if cores > 1:
        @pl.when(relaying & lead)
        def _():
            pl.semaphore_signal(go_sem, inc=1, device_id=partner, device_id_type=MESH)

    q_local.wait()
    for peer, _ in peers[1:]:
        wait_bytes(qbuf.at[at(peer * tok, tok)], q_recv.at[peer])

    def block(head, q_rows, key_rows, masked, first):
        q = qbuf[q_rows, head * HEAD_DIM : (head + 1) * HEAD_DIM]
        scores = lax.dot_general(
            q, kbuf[key_rows, :], (((1,), (1,)), ((), ())), preferred_element_type=jnp.float32
        ) * factor
        if masked:
            down = lax.broadcasted_iota(jnp.int32, scores.shape, 0)
            right = lax.broadcasted_iota(jnp.int32, scores.shape, 1)
            scores = jnp.where(right <= down, scores, masked_score)
        peak = jnp.max(scores, axis=1, keepdims=True)
        size = scores.shape[0]
        if first:
            new_top = jnp.broadcast_to(peak, (size, HEAD_DIM))
        else:
            old_top = top[head, q_rows]
            new_top = jnp.maximum(old_top, peak)
        repeats = scores.shape[1] // HEAD_DIM
        weights = jnp.exp2(scores - jnp.concatenate([new_top] * repeats, axis=1))
        if masked:
            weights = jnp.where(right <= down, weights, 0.0)
        part = weights[:, :HEAD_DIM]
        for r in range(1, repeats):
            part = part + weights[:, r * HEAD_DIM : (r + 1) * HEAD_DIM]
        mixed = jnp.dot(
            weights.astype(jnp.bfloat16), vbuf[key_rows, :], preferred_element_type=jnp.float32
        )
        if first:
            total[head, q_rows] = part
            summed[head, q_rows] = mixed
        else:
            shrink = jnp.exp2(old_top - new_top)
            total[head, q_rows] = total[head, q_rows] * shrink + part
            summed[head, q_rows] = summed[head, q_rows] * shrink + mixed
        top[head, q_rows] = new_top

    low, high = pl.ds(0, half_rows), pl.ds(half_rows, half_rows)
    own_low = at(slab * rows, half_rows)
    own_high = at(slab * rows + half_rows, half_rows)
    for head in range(GROUP):
        block(head, low, own_low, True, True)
        block(head, high, own_low, False, True)
        block(head, high, own_high, True, False)

    def visit(t, carry):
        @pl.when(t >= 2)
        def _():
            take(t)

        where = chunk_of(t)[2]
        for head in range(GROUP):
            for q_rows in (low, high):
                block(head, q_rows, where, False, False)
        return carry

    lax.fori_loop(0, 2 * slab - 1, visit, 0)
    last = 2 * slab - 1

    @pl.when(slab > 1)
    def _():
        take(last)

    def last_block(part):
        @pl.when(slab > 0)
        def _():
            where = chunk_of(last)[2]
            for head in range(GROUP):
                block(head, at(part * half_rows, half_rows), where, False, False)

    def finish(peer):
        where = at(peer * tok, tok)
        for head in range(GROUP):
            sums = jnp.sum(total[head, where], axis=1, keepdims=True)
            obuf[where, head * HEAD_DIM : (head + 1) * HEAD_DIM] = (
                summed[head, where] / sums
            ).astype(jnp.bfloat16)

    own_part = mine // (members // 2)
    last_block(1 - own_part)
    split = members // 2 if across == 2 else 1
    o_copies = []
    for i in reversed(range(1, members)):
        if i == split - 1 or (split == 1 and i == members - 1):
            last_block(own_part)
        peer, device = peers[i]
        finish(peer)
        copy = pltpu.make_async_remote_copy(
            src_ref=obuf.at[at(peer * tok, tok)],
            dst_ref=out_ref.at[:, cols(mine, width)],
            send_sem=o_send.at[i],
            recv_sem=o_recv.at[mine],
            device_id=device,
            device_id_type=MESH,
        )
        copy.start()
        o_copies.append(copy)
    finish(mine)
    o_local = pltpu.make_async_copy(
        obuf.at[at(mine * tok, tok)], out_ref.at[:, cols(mine, width)], local_sem.at[3]
    )
    o_local.start()

    for copy in kv_copies + q_copies:
        copy.wait_send()

    @pl.when(slab < slabs - 1)
    def _():
        for i in range(members):
            for copy in upward(i):
                copy.wait_send()

        def sent(t, carry):
            for copy in relay(t):
                copy.wait_send()
            return carry

        lax.fori_loop(0, 2 * slab, sent, 0)

    for copy in o_copies:
        copy.wait_send()
    o_local.wait()
    for peer, _ in peers[1:]:
        wait_bytes(out_ref.at[:, cols(peer, width)], o_recv.at[peer])


def solution(mesh):
    ulysses, blk = mesh.shape["ulysses"], mesh.shape["blk"]
    members = KV_HEADS
    assert members % blk == 0 and ulysses % (members // blk) == 0
    slabs = ulysses // (members // blk)

    def per_device(queries, key_rows, value_rows):
        tok = queries.shape[0]
        rows = members * tok
        seq = slabs * rows
        dma = pltpu.SemaphoreType.DMA
        return pl.pallas_call(
            functools.partial(kernel, ulysses, blk),
            out_shape=jax.ShapeDtypeStruct(queries.shape, queries.dtype),
            in_specs=[pl.BlockSpec(memory_space=pl.ANY)] * 3,
            out_specs=pl.BlockSpec(memory_space=pl.ANY),
            scratch_shapes=[
                pltpu.VMEM(queries.shape, queries.dtype),
                pltpu.VMEM(key_rows.shape, key_rows.dtype),
                pltpu.VMEM(value_rows.shape, value_rows.dtype),
                pltpu.VMEM((rows, GROUP * HEAD_DIM), jnp.bfloat16),
                pltpu.VMEM((seq, HEAD_DIM), jnp.bfloat16),
                pltpu.VMEM((seq, HEAD_DIM), jnp.bfloat16),
                pltpu.VMEM((rows, GROUP * HEAD_DIM), jnp.bfloat16),
                pltpu.VMEM((GROUP, rows, HEAD_DIM), jnp.float32),
                pltpu.VMEM((GROUP, rows, HEAD_DIM), jnp.float32),
                pltpu.VMEM((GROUP, rows, HEAD_DIM), jnp.float32),
                dma((7,)),
                dma((members, 2)),
                dma((members, 2)),
                dma((members,)),
                dma((members,)),
                dma((members, 2)),
                dma((slabs, 2, 2)),
                dma((slabs, 2, 2)),
                dma((members,)),
                dma((members,)),
                pltpu.SemaphoreType.REGULAR,
            ],
            compiler_params=pltpu.CompilerParams(collective_id=0, has_side_effects=True),
        )(queries, key_rows, value_rows)

    spec = P(("ulysses", "blk"), None)
    return jax.shard_map(
        per_device, mesh=mesh, in_specs=(spec, spec, spec), out_specs=spec, check_vma=False
    )
```
